128 devices in a mesh: ctx: 16 (over z_lo, x, core), tp: 8 (over y, z_hi).
Axes of the slice: x: 4, y: 4, z: 4 (z_hi: 2, z_lo: 2; z = z_hi * 2 + z_lo), core: 2. Of those that a mesh axis runs over, the one named last changes fastest.
Arguments:
- queries: bfloat16 [2048, 16384], P('ctx', 'tp'), may hold values from -110 to 110
- key_value_cache: bfloat16 [2, 10240, 1024], P(None, 'ctx', 'tp'), may hold values from -9 to 9
- cache_lengths: int32 [16], P('ctx'), may hold values from 64 to 512, as said below
- token_order: int32 [2048], P('ctx'), may hold values from 0 to 2047, each once
- out_weight: bfloat16 [16384, 16384], P('tp', 'ctx'), may hold values from -0.046875 to 0.046875
Outputs:
- output: bfloat16 [2048, 16384], P('tp', 'ctx')
The draws below stay inside these ranges and needn't reach their ends.
Inputs may be any that keep to these rules, and one draw needn't show every extreme that they name: `cache_lengths`: one shard's cache is full in every draw. `token_order`: each number of 0 to 2047 stands once.
All inputs are finite; a program needn't handle non-finite values.
Results may differ from the reference program's by a relative error of at most 0.04.
Values may be sent and summed in bfloat16 or wider, within the bound.
No kernel may reach another device: no remote copies, remote signals or barrier semaphores. Data moves between devices by JAX's collectives and lax.ppermute only.
A program may use at most 64 MiB of HBM per device.

```python
import math
import jax
import jax.numpy as jnp
from jax import lax

D = 16384
QUERY_HEADS = 128
KEY_VALUE_HEADS = 8
HEAD_SIZE = 128
TOKENS_PER_SHARD = 128
CACHE_DEV = 512
SHARD_ROWS = 640
NEW_TOKENS = 2048
KEY_VALUE_ROWS = 10240
N_CTX = 16


def shared_tensors(key):
    key_entries, value_entries, key_queries = jax.random.split(jax.random.fold_in(key, 7), 3)
    key_matrix = jnp.clip(jax.random.normal(key_entries, (KEY_VALUE_ROWS, KEY_VALUE_HEADS * HEAD_SIZE), jnp.float32), -4.5, 4.5)
    value_matrix = jnp.clip(jax.random.normal(value_entries, (KEY_VALUE_ROWS, KEY_VALUE_HEADS * HEAD_SIZE), jnp.float32), -4.5, 4.5)
    queries = 3.0 * jnp.clip(jax.random.normal(key_queries, (NEW_TOKENS, QUERY_HEADS * HEAD_SIZE), jnp.float32), -6.0, 6.0)
    return (queries, key_matrix, value_matrix)


def draw_queries(key, part):
    queries, key_matrix, value_matrix = shared_tensors(key)
    return queries.astype(jnp.bfloat16)


def draw_key_value_cache(key, part):
    queries, key_matrix, value_matrix = shared_tensors(key)
    return jnp.stack([key_matrix, value_matrix]).astype(jnp.bfloat16)


def draw_cache_lengths(key, part):
    first, second_part = jax.random.split(jax.random.fold_in(key, 11))
    shards = KEY_VALUE_ROWS // SHARD_ROWS
    lengths = jax.random.randint(first, (shards,), max(2, CACHE_DEV // 8), CACHE_DEV // 2 + 1)
    fullest = jax.random.randint(second_part, (), 0, shards)
    return jnp.where(jnp.arange(shards) == fullest, CACHE_DEV, lengths).astype(jnp.int32)


def level_of(stream_key, extent, pieces, smallest, high):
    def one(position, parts):
        heights = jax.random.uniform(jax.random.fold_in(jax.random.fold_in(stream_key, 6), position), (parts,), jnp.float32, smallest / len(pieces), high / len(pieces))
        return jnp.repeat(jnp.exp(heights), extent[position] // parts).reshape((-1,) + (1,) * (len(extent) - position - 1))

    gain = one(*pieces[0])
    for cut in pieces[1:]:
        gain = gain * one(*cut)
    return gain


def noise(own_key, shape, scale, limit, pieces=(), held_as=jnp.bfloat16):
    loudness = level_of(own_key, shape, pieces, -0.22, 0.18) if pieces else 1.0
    array = jax.random.normal(own_key, shape, jnp.float32) * scale * loudness
    return jnp.minimum(jnp.maximum(array, -limit), limit).astype(held_as)


def setup_inputs(seed: int = 0) -> dict:
    key_list = jax.random.split(jax.random.key(seed), 6)
    queries = draw_queries(jax.random.fold_in(key_list[5], 71), 0)
    key_value_cache = draw_key_value_cache(jax.random.fold_in(key_list[5], 71), 0)
    cache_lengths = draw_cache_lengths(jax.random.fold_in(key_list[5], 71), 0)
    token_order = jax.random.permutation(key_list[3], NEW_TOKENS).astype(jnp.int32)
    out_weight = noise(key_list[4], (QUERY_HEADS * HEAD_SIZE, D), (QUERY_HEADS * HEAD_SIZE) ** -0.5, 0.046875, ((0, 8), (1, 16)))
    return dict(queries=queries, key_value_cache=key_value_cache, cache_lengths=cache_lengths, token_order=token_order, out_weight=out_weight)


def reference(queries, key_value_cache, cache_lengths, token_order, out_weight):
    group_index = QUERY_HEADS // KEY_VALUE_HEADS
    scale = 1.0 / math.sqrt(HEAD_SIZE)
    within = jnp.arange(SHARD_ROWS, dtype=jnp.int32)
    cache_valid = (within[None, :] < cache_lengths[:, None]) & (within[None, :] < CACHE_DEV)
    latest = jnp.full((N_CTX, CACHE_DEV), NEW_TOKENS, jnp.int32)
    key_order = jnp.concatenate([latest, token_order.reshape(N_CTX, TOKENS_PER_SHARD).astype(jnp.int32)], axis=1)
    cache_valid = cache_valid.reshape(KEY_VALUE_ROWS)
    key_order = key_order.reshape(KEY_VALUE_ROWS)
    key_matrix = jnp.transpose(key_value_cache[0].astype(jnp.float32).reshape(KEY_VALUE_ROWS, KEY_VALUE_HEADS, HEAD_SIZE), (1, 0, 2))
    value_matrix = jnp.transpose(key_value_cache[1].astype(jnp.float32).reshape(KEY_VALUE_ROWS, KEY_VALUE_HEADS, HEAD_SIZE), (1, 0, 2))
    block_list = queries.reshape(N_CTX, TOKENS_PER_SHARD, KEY_VALUE_HEADS, group_index, HEAD_SIZE)
    orders = token_order.reshape(N_CTX, TOKENS_PER_SHARD).astype(jnp.int32)

    def one_block(pair):
        block_slice, order = pair
        allowed = cache_valid[None, :] | (key_order[None, :] <= order[:, None])

        def one_head(triple):
            heads, head_keys, head_values = triple
            scores = jnp.einsum('tgd,nd->gtn', heads.astype(jnp.float32), head_keys) * scale
            scores = jnp.where(allowed[None], scores, -jnp.inf)
            peak = lax.optimization_barrier(jnp.max(scores, axis=-1, keepdims=True))
            raised = jnp.exp(scores - peak)
            total = lax.optimization_barrier(jnp.sum(raised, axis=-1, keepdims=True))
            weights = lax.optimization_barrier(raised.astype(jnp.bfloat16)).astype(jnp.float32)
            return jnp.einsum('gtn,nd->gtd', weights, head_values) / total
        mixed = lax.map(one_head, (jnp.transpose(block_slice, (1, 0, 2, 3)), key_matrix, value_matrix))
        return jnp.transpose(mixed, (2, 0, 1, 3)).reshape(TOKENS_PER_SHARD, QUERY_HEADS * HEAD_SIZE).astype(jnp.bfloat16)
    attended = lax.map(one_block, (block_list, orders)).reshape(NEW_TOKENS, QUERY_HEADS * HEAD_SIZE)
    return jnp.dot(attended, out_weight, preferred_element_type=jnp.float32).astype(jnp.bfloat16)
```

```python
import math
import jax
import jax.numpy as jnp
from jax import lax
from jax.sharding import Mesh
from jax.sharding import PartitionSpec as P
from jax.experimental import pallas as pl
from jax.experimental.pallas import tpu as pltpu

HEAD_SIZE = 128
UNIT = 128
BLOCK = 512
TILE = 256
CACHE_DEV = 512
SHARD_ROWS = 640
SHARDS = 16
V_ROWS = 144
FLOOR = -1e30
TO_EXP2 = math.log2(math.e) / math.sqrt(HEAD_SIZE)


def attend_kernel(lens, order, own, q, kv, out, keys, values, queries, peak, acc):
    heads = q.shape[1] // HEAD_SIZE
    unit_rows = lax.broadcasted_iota(jnp.int32, (UNIT, HEAD_SIZE), 0)
    v_rows = lax.broadcasted_iota(jnp.int32, (V_ROWS - HEAD_SIZE, UNIT), 0)
    v_lanes = lax.broadcasted_iota(jnp.int32, (V_ROWS - HEAD_SIZE, UNIT), 1)
    lanes = lax.broadcasted_iota(jnp.int32, (HEAD_SIZE, UNIT), 1)

    for h in range(heads):
        queries[:, h * UNIT:(h + 1) * UNIT] = q[:, h * HEAD_SIZE:(h + 1) * HEAD_SIZE].T

    def put(at, key_unit, value_unit, left):
        keys[pl.ds(at, UNIT), :] = key_unit
        values[:HEAD_SIZE, pl.ds(at, UNIT)] = jnp.where(lanes < left, value_unit, 0).astype(jnp.bfloat16)
        values[HEAD_SIZE:, pl.ds(at, UNIT)] = jnp.where((v_rows == 0) & (v_lanes < left), 1.0, 0.0).astype(jnp.bfloat16)

    def fresh_unit(s, carry):
        at = pl.multiple_of(s * SHARD_ROWS + CACHE_DEV, UNIT)
        put(pl.multiple_of(s * UNIT, UNIT), kv[0, pl.ds(at, UNIT), :], kv[1, pl.ds(at, UNIT), :].T, UNIT)
        return carry

    lax.fori_loop(0, SHARDS, fresh_unit, 0)

    def shard_units(s, used):
        base = pl.multiple_of(s * SHARD_ROWS, UNIT)
        length = lens[s]
        first = jnp.broadcast_to(kv[0, pl.ds(base, 16), :][:1], (UNIT, HEAD_SIZE))

        def unit(b, used):
            at = pl.multiple_of(base + b * UNIT, UNIT)
            left = length - b * UNIT
            key_unit = jnp.where(unit_rows < left, kv[0, pl.ds(at, UNIT), :], first)
            put(pl.multiple_of(used, UNIT), key_unit, kv[1, pl.ds(at, UNIT), :].T, left)
            return used + UNIT

        return lax.fori_loop(0, (length + UNIT - 1) // UNIT, unit, used)

    used = lax.fori_loop(0, SHARDS, shard_units, SHARDS * UNIT)
    blocks = (used + BLOCK - 1) // BLOCK
    spare = jnp.broadcast_to(kv[0, 0:16, :][:1], (UNIT, HEAD_SIZE))
    nothing = jnp.zeros((HEAD_SIZE, UNIT), jnp.bfloat16)

    def pad(i, carry):
        put(pl.multiple_of(used + i * UNIT, UNIT), spare, nothing, 0)
        return carry

    lax.fori_loop(0, (blocks * BLOCK - used) // UNIT, pad, 0)

    peak[...] = jnp.full(peak.shape, FLOOR, jnp.float32)
    acc[...] = jnp.zeros(acc.shape, jnp.float32)

    def absorb(at, allowed):
        key_block = keys[pl.ds(at, BLOCK), :]
        value_block = values[:, pl.ds(at, BLOCK)]
        for t in range(heads * UNIT // TILE):
            cols = slice(t * TILE, (t + 1) * TILE)
            scores = jnp.dot(key_block, queries[:, cols], preferred_element_type=jnp.float32)
            if allowed is not None:
                scores = jnp.where(allowed, scores, FLOOR)
            old = peak[:, cols]
            new = jnp.maximum(old, jnp.max(scores, axis=0, keepdims=True))
            weights = jnp.exp2((scores - new) * TO_EXP2).astype(jnp.bfloat16)
            acc[:, cols] = acc[:, cols] * jnp.exp2((old - new) * TO_EXP2) + jnp.dot(
                value_block, weights, preferred_element_type=jnp.float32
            )
            peak[:, cols] = new

    def cache_block(i, carry):
        absorb(pl.multiple_of(i * BLOCK, BLOCK), None)
        return carry

    lax.fori_loop(SHARDS * UNIT // BLOCK, blocks, cache_block, 0)

    own_row = own[...]

    def fresh_block(i, carry):
        rows = []
        for j in range(BLOCK // UNIT):
            row = order[pl.ds(i * (BLOCK // UNIT) + j, 1), :]
            rows.append(jnp.broadcast_to(row, (UNIT, UNIT)).T)
        column = jnp.concatenate(rows, axis=0)
        allowed = column <= own_row
        allowed = jnp.concatenate([allowed] * (TILE // UNIT), axis=1)
        absorb(pl.multiple_of(i * BLOCK, BLOCK), allowed)
        return carry

    lax.fori_loop(0, SHARDS * UNIT // BLOCK, fresh_block, 0)

    for h in range(heads):
        cols = slice(h * UNIT, (h + 1) * UNIT)
        done = acc[:HEAD_SIZE, cols] / acc[HEAD_SIZE:HEAD_SIZE + 1, cols]
        out[:, h * HEAD_SIZE:(h + 1) * HEAD_SIZE] = done.T.astype(jnp.bfloat16)


def attend(lens, order, own, q, kv):
    rows = kv.shape[1]
    width = q.shape[1]
    vmem = pl.BlockSpec(memory_space=pltpu.VMEM)
    return pl.pallas_call(
        attend_kernel,
        out_shape=jax.ShapeDtypeStruct(q.shape, jnp.bfloat16),
        in_specs=[pl.BlockSpec(memory_space=pltpu.SMEM), vmem, vmem, vmem, vmem],
        out_specs=vmem,
        scratch_shapes=[
            pltpu.VMEM((rows, HEAD_SIZE), jnp.bfloat16),
            pltpu.VMEM((V_ROWS, rows), jnp.bfloat16),
            pltpu.VMEM((HEAD_SIZE, width), jnp.bfloat16),
            pltpu.VMEM((1, width), jnp.float32),
            pltpu.VMEM((V_ROWS, width), jnp.float32),
        ],
        compiler_params=pltpu.CompilerParams(vmem_limit_bytes=48 * 2**20),
    )(lens, order, own, q, kv)


TP = ("tp_0", "tp_1")
TOKENS_PER_SHARD = 128


def body(queries, key_value_cache, cache_lengths, token_order, out_weight):
    gathered = lax.all_gather(key_value_cache, "ctx", axis=1, tiled=True)
    facts = jnp.concatenate([token_order, jnp.broadcast_to(cache_lengths, (128,))])[None]
    facts = lax.all_gather(facts, "ctx", axis=0, tiled=True)
    attended = attend(facts[:, 128], facts[:, :128].astype(jnp.float32), token_order[None].astype(jnp.float32), queries, gathered)
    terms = jnp.dot(
        lax.all_gather(attended, "ctx", axis=0, tiled=True),
        out_weight,
        preferred_element_type=jnp.float32,
    ).astype(jnp.bfloat16)
    terms = lax.psum_scatter(terms, "tp_0", scatter_dimension=0, tiled=True)
    return lax.psum_scatter(terms, "tp_1", scatter_dimension=0, tiled=True)


def solution(mesh):
    torus = Mesh(mesh.devices.reshape(mesh.shape["ctx"], 4, 2), ("ctx", "tp_0", "tp_1"))
    return jax.shard_map(
        body,
        mesh=torus,
        in_specs=(P("ctx", TP), P(None, "ctx", TP), P("ctx"), P("ctx"), P(TP, "ctx")),
        out_specs=P(TP, "ctx"),
        check_vma=False,
    )
```

```python
import math
import jax
import jax.numpy as jnp
from jax import lax
from jax.sharding import Mesh
from jax.sharding import PartitionSpec as P
from jax.experimental import pallas as pl
from jax.experimental.pallas import tpu as pltpu

HEAD_SIZE = 128
UNIT = 128
BLOCK = 512
TILE = 256
CACHE_DEV = 512
SHARD_ROWS = 640
SHARDS = 16
V_ROWS = 144
FLOOR = -1e30
TO_EXP2 = math.log2(math.e) / math.sqrt(HEAD_SIZE)


def attend_kernel(lens, order, own, q, kv, low, high, keys, values, queries, peak, acc):
    heads = q.shape[1] // HEAD_SIZE
    unit_rows = lax.broadcasted_iota(jnp.int32, (UNIT, HEAD_SIZE), 0)
    v_rows = lax.broadcasted_iota(jnp.int32, (V_ROWS - HEAD_SIZE, UNIT), 0)
    v_lanes = lax.broadcasted_iota(jnp.int32, (V_ROWS - HEAD_SIZE, UNIT), 1)
    lanes = lax.broadcasted_iota(jnp.int32, (HEAD_SIZE, UNIT), 1)

    for h in range(heads):
        queries[:, h * UNIT:(h + 1) * UNIT] = q[:, h * HEAD_SIZE:(h + 1) * HEAD_SIZE].T

    def put(at, key_unit, value_unit, left):
        keys[pl.ds(at, UNIT), :] = key_unit
        values[:HEAD_SIZE, pl.ds(at, UNIT)] = jnp.where(lanes < left, value_unit, 0).astype(jnp.bfloat16)
        values[HEAD_SIZE:, pl.ds(at, UNIT)] = jnp.where((v_rows == 0) & (v_lanes < left), 1.0, 0.0).astype(jnp.bfloat16)

    def fresh_unit(s, carry):
        at = pl.multiple_of(s * SHARD_ROWS + CACHE_DEV, UNIT)
        put(pl.multiple_of(s * UNIT, UNIT), kv[0, pl.ds(at, UNIT), :], kv[1, pl.ds(at, UNIT), :].T, UNIT)
        return carry

    lax.fori_loop(0, SHARDS, fresh_unit, 0)

    def shard_units(s, used):
        base = pl.multiple_of(s * SHARD_ROWS, UNIT)
        length = lens[s]
        first = jnp.broadcast_to(kv[0, pl.ds(base, 16), :][:1], (UNIT, HEAD_SIZE))

        def unit(b, used):
            at = pl.multiple_of(base + b * UNIT, UNIT)
            left = length - b * UNIT
            key_unit = jnp.where(unit_rows < left, kv[0, pl.ds(at, UNIT), :], first)
            put(pl.multiple_of(used, UNIT), key_unit, kv[1, pl.ds(at, UNIT), :].T, left)
            return used + UNIT

        return lax.fori_loop(0, (length + UNIT - 1) // UNIT, unit, used)

    used = lax.fori_loop(0, SHARDS, shard_units, SHARDS * UNIT)
    blocks = (used + BLOCK - 1) // BLOCK
    spare = jnp.broadcast_to(kv[0, 0:16, :][:1], (UNIT, HEAD_SIZE))
    nothing = jnp.zeros((HEAD_SIZE, UNIT), jnp.bfloat16)

    def pad(i, carry):
        put(pl.multiple_of(used + i * UNIT, UNIT), spare, nothing, 0)
        return carry

    lax.fori_loop(0, (blocks * BLOCK - used) // UNIT, pad, 0)

    peak[...] = jnp.full(peak.shape, FLOOR, jnp.float32)
    acc[...] = jnp.zeros(acc.shape, jnp.float32)

    def absorb(at, allowed):
        key_block = keys[pl.ds(at, BLOCK), :]
        value_block = values[:, pl.ds(at, BLOCK)]
        for t in range(heads * UNIT // TILE):
            cols = slice(t * TILE, (t + 1) * TILE)
            scores = jnp.dot(key_block, queries[:, cols], preferred_element_type=jnp.float32)
            if allowed is not None:
                scores = jnp.where(allowed, scores, FLOOR)
            old = peak[:, cols]
            new = jnp.maximum(old, jnp.max(scores, axis=0, keepdims=True))
            weights = jnp.exp2((scores - new) * TO_EXP2).astype(jnp.bfloat16)
            acc[:, cols] = acc[:, cols] * jnp.exp2((old - new) * TO_EXP2) + jnp.dot(
                value_block, weights, preferred_element_type=jnp.float32
            )
            peak[:, cols] = new

    def cache_block(i, carry):
        absorb(pl.multiple_of(i * BLOCK, BLOCK), None)
        return carry

    lax.fori_loop(SHARDS * UNIT // BLOCK, blocks, cache_block, 0)

    own_row = own[...]

    def fresh_block(i, carry):
        rows = []
        for j in range(BLOCK // UNIT):
            row = order[pl.ds(i * (BLOCK // UNIT) + j, 1), :]
            rows.append(jnp.broadcast_to(row, (UNIT, UNIT)).T)
        column = jnp.concatenate(rows, axis=0)
        allowed = column <= own_row
        allowed = jnp.concatenate([allowed] * (TILE // UNIT), axis=1)
        absorb(pl.multiple_of(i * BLOCK, BLOCK), allowed)
        return carry

    lax.fori_loop(0, SHARDS * UNIT // BLOCK, fresh_block, 0)

    for h in range(heads):
        cols = slice(h * UNIT, (h + 1) * UNIT)
        done = acc[:HEAD_SIZE, cols] / acc[HEAD_SIZE:HEAD_SIZE + 1, cols]
        done = done.T.astype(jnp.bfloat16)
        low[:, h * HEAD_SIZE:(h + 1) * HEAD_SIZE] = done[:HALF]
        high[:, h * HEAD_SIZE:(h + 1) * HEAD_SIZE] = done[HALF:]


def attend(lens, order, own, q, kv):
    rows = kv.shape[1]
    width = q.shape[1]
    vmem = pl.BlockSpec(memory_space=pltpu.VMEM)
    return pl.pallas_call(
        attend_kernel,
        out_shape=[jax.ShapeDtypeStruct((HALF, width), jnp.bfloat16)] * 2,
        in_specs=[pl.BlockSpec(memory_space=pltpu.SMEM), vmem, vmem, vmem, vmem],
        out_specs=[vmem, vmem],
        scratch_shapes=[
            pltpu.VMEM((rows, HEAD_SIZE), jnp.bfloat16),
            pltpu.VMEM((V_ROWS, rows), jnp.bfloat16),
            pltpu.VMEM((HEAD_SIZE, width), jnp.bfloat16),
            pltpu.VMEM((1, width), jnp.float32),
            pltpu.VMEM((V_ROWS, width), jnp.float32),
        ],
        compiler_params=pltpu.CompilerParams(vmem_limit_bytes=48 * 2**20),
    )(lens, order, own, q, kv)


AXES = ("zl", "x", "core", "y", "zh")
HALF = 64


def turn(axis_value, axis, by, size):
    return lax.ppermute(axis_value, axis, [(i, (i + by) % size) for i in range(size)])


def gather_shards(own):
    rows = own.shape[0] // 2
    left = turn(own, "x", 1, 4)
    right = turn(own, "x", 3, 4)
    above = turn(own, "zl", 1, 2)
    far_low = turn(left[:rows], "x", 1, 4)
    far_high = turn(right[rows:], "x", 3, 4)
    above_left = turn(above, "x", 1, 4)
    above_right = turn(above, "x", 3, 4)
    above_far_low = turn(far_low, "zl", 1, 2)
    above_far_high = turn(far_high, "zl", 1, 2)
    return (own, left, right, far_low, far_high, above, above_left, above_right, above_far_low, above_far_high)


def project_kernel(place, *refs):
    *shards, weight, out, joined = refs
    tokens = shards[0].shape[0]
    for ref, (spot, begin) in zip(shards, SHARD_SPOTS):
        at = pl.multiple_of(place[spot] * tokens + begin * (tokens // 2), 16)
        joined[pl.ds(at, ref.shape[0]), :] = ref[...]
    out[...] = jnp.dot(joined[...], weight[...], preferred_element_type=jnp.float32).astype(jnp.bfloat16)


SHARD_SPOTS = ((0, 0), (1, 0), (2, 0), (3, 0), (3, 1), (4, 0), (5, 0), (6, 0), (7, 0), (7, 1))


def project(place, shards, weight):
    tokens = 8 * shards[0].shape[0]
    vmem = pl.BlockSpec(memory_space=pltpu.VMEM)
    return pl.pallas_call(
        project_kernel,
        out_shape=jax.ShapeDtypeStruct((tokens, weight.shape[1]), jnp.bfloat16),
        in_specs=[pl.BlockSpec(memory_space=pltpu.SMEM)] + [vmem] * (len(shards) + 1),
        out_specs=vmem,
        scratch_shapes=[pltpu.VMEM((tokens, weight.shape[0]), jnp.bfloat16)],
        cost_estimate=pl.CostEstimate(
            flops=2 * tokens * weight.shape[0] * weight.shape[1],
            bytes_accessed=2 * (tokens + weight.shape[1]) * weight.shape[0],
            transcendentals=0,
        ),
        compiler_params=pltpu.CompilerParams(vmem_limit_bytes=40 * 2**20),
    )(place, *shards, weight)


def scatter_sum(terms, y, zh):
    pieces = terms.reshape(4, 2, -1, terms.shape[1])

    def piece(k):
        return lax.dynamic_index_in_dim(pieces, (y + k) % 4, 0, keepdims=False)

    parts = [turn(piece(k), "y", k, 4) for k in (1, 3, 2)]
    total = piece(0).astype(jnp.float32)
    for part in parts:
        total = total + part.astype(jnp.float32)
    away = turn(lax.dynamic_index_in_dim(total, 1 - zh, 0, keepdims=False).astype(jnp.bfloat16), "zh", 1, 2)
    kept = lax.dynamic_index_in_dim(total, zh, 0, keepdims=False)
    return (kept + away.astype(jnp.float32)).astype(jnp.bfloat16)


def body(queries, key_value_cache, cache_lengths, token_order, out_weight):
    zl, x, core, y, zh = (lax.axis_index(name) for name in AXES)
    ctx = ("zl", "x", "core")
    gathered = lax.all_gather(key_value_cache, ctx, axis=1, tiled=True)
    facts = jnp.concatenate([token_order, jnp.broadcast_to(cache_lengths, (128,))])[None]
    facts = lax.all_gather(facts, ctx, axis=0, tiled=True)
    other_weight = turn(out_weight, "core", 1, 2)
    halves = attend(facts[:, 128], facts[:, :128].astype(jnp.float32), token_order[None].astype(jnp.float32), queries, gathered)
    rows = [zl * 4 + (x + d) % 4 for d in (0, 3, 1, 2)]
    place = jnp.stack(rows + [(row + 4) % 8 for row in rows]).astype(jnp.int32)
    own_parts, other_parts = [], []
    for half in halves:
        shards = gather_shards(half)
        other_parts.append(turn(scatter_sum(project(place, shards, other_weight), y, zh), "core", 1, 2))
        own_parts.append(scatter_sum(project(place, shards, out_weight), y, zh))
    own_rows = jnp.concatenate(own_parts, axis=0)
    other_rows = jnp.concatenate(other_parts, axis=0)
    first = jnp.where(core == 0, own_rows, other_rows)
    second = jnp.where(core == 0, other_rows, own_rows)
    return jnp.concatenate([first, second], axis=0)


def solution(mesh):
    torus = Mesh(mesh.devices.reshape(2, 4, 2, 4, 2), AXES)
    ctx, tp = ("zl", "x", "core"), ("y", "zh")
    return jax.shard_map(
        body,
        mesh=torus,
        in_specs=(P(ctx, tp), P(None, ctx, tp), P(ctx), P(ctx), P(tp, ctx)),
        out_specs=P(tp, ctx),
        check_vma=False,
    )
```

```python
import math
import jax
import jax.numpy as jnp
from jax import lax
from jax.sharding import Mesh
from jax.sharding import PartitionSpec as P
from jax.experimental import pallas as pl
from jax.experimental.pallas import tpu as pltpu

HEAD_SIZE = 128
UNIT = 128
BLOCK = 512
CACHE_DEV = 512
SHARD_ROWS = 640
PACKED_ROWS = 656
V_ROWS = 144
HALF = 64
FLOOR = -1e30
NEVER = 1e9
TO_EXP2 = math.log2(math.e) / math.sqrt(HEAD_SIZE)


def whole(ref):
    return ref.at[0], ref.at[1]


def fill(shards, keys, values, marks):
    value_rows = lax.broadcasted_iota(jnp.int32, (V_ROWS - HEAD_SIZE, values.shape[1]), 0)
    values[HEAD_SIZE:, :] = jnp.where(value_rows == 0, 1.0, 0.0).astype(jnp.bfloat16)
    lanes = lax.broadcasted_iota(jnp.int32, (1, UNIT), 1).astype(jnp.float32)
    used = 0
    for key_ref, value_ref in shards:
        facts = key_ref[SHARD_ROWS:, :].astype(jnp.float32)
        length = facts[2:3] * 64.0 + facts[3:4]
        count = jnp.max((length + (UNIT - 1.0)) * (1.0 / UNIT)).astype(jnp.int32)

        def unit(b, used, key_ref=key_ref, value_ref=value_ref, length=length):
            begin = pl.multiple_of(b * UNIT, UNIT)
            at = pl.multiple_of(used * UNIT, UNIT)
            keys[pl.ds(at, UNIT), :] = key_ref[pl.ds(begin, UNIT), :]
            values[:HEAD_SIZE, pl.ds(at, UNIT)] = value_ref[pl.ds(begin, UNIT), :].T
            marks[pl.ds(used, 1), :] = jnp.where(lanes + (b * UNIT).astype(jnp.float32) < length, -1.0, NEVER)
            return used + 1

        used = lax.fori_loop(0, count, unit, used)
        at = pl.multiple_of(used * UNIT, UNIT)
        keys[pl.ds(at, UNIT), :] = key_ref[CACHE_DEV:SHARD_ROWS, :]
        values[:HEAD_SIZE, pl.ds(at, UNIT)] = value_ref[CACHE_DEV:SHARD_ROWS, :].T
        marks[pl.ds(used, 1), :] = facts[0:1] * 64.0 + facts[1:2]
        used = used + 1
    per_block = BLOCK // UNIT
    blocks = (used + per_block - 1) // per_block

    def spare(i, carry):
        at = pl.multiple_of(i * UNIT, UNIT)
        keys[pl.ds(at, UNIT), :] = jnp.zeros((UNIT, HEAD_SIZE), jnp.bfloat16)
        values[:HEAD_SIZE, pl.ds(at, UNIT)] = jnp.zeros((HEAD_SIZE, UNIT), jnp.bfloat16)
        marks[pl.ds(i, 1), :] = jnp.full((1, UNIT), NEVER, jnp.float32)
        return carry

    lax.fori_loop(used, blocks * per_block, spare, 0)
    return blocks


def absorb_all(blocks, keys, values, marks, own_rows, queries, begin, peak, acc):
    width = peak.shape[1]
    half_width = queries.shape[1] // 2

    def block(i, carry):
        at = pl.multiple_of(i * BLOCK, BLOCK)
        key_block = keys[pl.ds(at, BLOCK), :]
        value_block = values[:, pl.ds(at, BLOCK)]
        columns = [
            jnp.broadcast_to(marks[pl.ds(i * (BLOCK // UNIT) + j, 1), :], (UNIT, UNIT)).T for j in range(BLOCK // UNIT)
        ]
        column = jnp.concatenate(columns, axis=0)
        allowed = [column <= row for row in own_rows]
        scores = jnp.dot(key_block, queries[:, begin:begin + width], preferred_element_type=jnp.float32)
        pieces = []
        for t in range(width // UNIT):
            which = allowed[(t * UNIT) // half_width if width > half_width else 0]
            pieces.append(jnp.where(which, scores[:, t * UNIT:(t + 1) * UNIT], FLOOR))
        scores = jnp.concatenate(pieces, axis=1)
        old = peak[...]
        new = jnp.maximum(old, jnp.max(scores, axis=0, keepdims=True))
        weights = jnp.exp2((scores - new) * TO_EXP2).astype(jnp.bfloat16)
        acc[...] = acc[...] * jnp.exp2((old - new) * TO_EXP2) + jnp.dot(
            value_block, weights, preferred_element_type=jnp.float32
        )
        peak[...] = new
        return carry

    lax.fori_loop(0, blocks, block, 0)


def first_kernel(own, q, s0, s1, s2, s3, s4, s5, s6, s7, queries, peak, acc, keys, values, marks):
    heads = q.shape[1] // HEAD_SIZE
    for half in range(2):
        for h in range(0, heads, 2):
            rows = slice(half * HALF, (half + 1) * HALF)
            pair = jnp.concatenate(
                [q[rows, h * HEAD_SIZE:(h + 1) * HEAD_SIZE], q[rows, (h + 1) * HEAD_SIZE:(h + 2) * HEAD_SIZE]], axis=0
            )
            at = half * heads * HALF + h * HALF
            queries[:, at:at + UNIT] = pair.T
    peak[...] = jnp.full(peak.shape, FLOOR, jnp.float32)
    acc[...] = jnp.zeros(acc.shape, jnp.float32)
    blocks = fill([whole(s) for s in (s0, s1, s2, s3, s4, s5, s6, s7)], keys, values, marks)
    absorb_all(blocks, keys, values, marks, (own[0:1], own[1:2]), queries, 0, peak, acc)


def finish(acc, out):
    for p in range(acc.shape[1] // UNIT):
        cols = slice(p * UNIT, (p + 1) * UNIT)
        done = (acc[:HEAD_SIZE, cols] / acc[HEAD_SIZE:HEAD_SIZE + 1, cols]).T.astype(jnp.bfloat16)
        out[:, (2 * p) * HEAD_SIZE:(2 * p + 1) * HEAD_SIZE] = done[:HALF]
        out[:, (2 * p + 1) * HEAD_SIZE:(2 * p + 2) * HEAD_SIZE] = done[HALF:]


def second_kernel(own, queries, peak_in, acc_in, s0, s1, s2, s3, s4, s5, k6, v6, k7, v7,
                  out, keys, values, marks, blocks_out, peak, acc):
    width = peak.shape[1]
    peak[...] = peak_in[:, :width]
    acc[...] = acc_in[:, :width]
    shards = [whole(s) for s in (s0, s1, s2, s3, s4, s5)] + [(k6, v6), (k7, v7)]
    blocks = fill(shards, keys, values, marks)
    blocks_out[0] = blocks
    absorb_all(blocks, keys, values, marks, (own[0:1],), queries, 0, peak, acc)
    finish(acc, out)


def third_kernel(blocks, own, queries, peak_in, acc_in, keys, values, marks, out, peak, acc):
    width = peak.shape[1]
    peak[...] = peak_in[:, width:]
    acc[...] = acc_in[:, width:]
    absorb_all(blocks[0], keys, values, marks, (own[1:2],), queries, width, peak, acc)
    finish(acc, out)


def attend(own, q, near, far):
    width = q.shape[1]
    units = 8 * SHARD_ROWS // UNIT
    vmem = pl.BlockSpec(memory_space=pltpu.VMEM)
    smem = pl.BlockSpec(memory_space=pltpu.SMEM)
    params = pltpu.CompilerParams(vmem_limit_bytes=48 * 2**20)
    store = [
        jax.ShapeDtypeStruct((units * UNIT, HEAD_SIZE), jnp.bfloat16),
        jax.ShapeDtypeStruct((V_ROWS, units * UNIT), jnp.bfloat16),
        jax.ShapeDtypeStruct((units, UNIT), jnp.float32),
    ]
    store_scratch = [pltpu.VMEM(s.shape, s.dtype) for s in store]

    def cost(queries_done):
        return pl.CostEstimate(
            flops=4 * queries_done * (units // 2) * UNIT * HEAD_SIZE * 2,
            bytes_accessed=4 * 2**20,
            transcendentals=queries_done * (units // 2) * UNIT,
        )

    queries, peak, acc = pl.pallas_call(
        first_kernel,
        out_shape=[
            jax.ShapeDtypeStruct((HEAD_SIZE, width), jnp.bfloat16),
            jax.ShapeDtypeStruct((1, width), jnp.float32),
            jax.ShapeDtypeStruct((V_ROWS, width), jnp.float32),
        ],
        in_specs=[vmem] * 10,
        out_specs=[vmem] * 3,
        scratch_shapes=store_scratch,
        cost_estimate=cost(width),
        compiler_params=params,
        name="attend_near",
    )(own, q, *near)
    half = jax.ShapeDtypeStruct((HALF, width), jnp.bfloat16)
    state_scratch = [pltpu.VMEM((1, width // 2), jnp.float32), pltpu.VMEM((V_ROWS, width // 2), jnp.float32)]
    low, keys, values, marks, blocks = pl.pallas_call(
        second_kernel,
        out_shape=[half] + store + [jax.ShapeDtypeStruct((1,), jnp.int32)],
        in_specs=[vmem] * 14,
        out_specs=[vmem] * 4 + [smem],
        scratch_shapes=state_scratch,
        cost_estimate=cost(width // 2),
        compiler_params=params,
        name="attend_far_low",
    )(own, queries, peak, acc, *far)
    high = pl.pallas_call(
        third_kernel,
        out_shape=half,
        in_specs=[smem] + [vmem] * 7,
        out_specs=vmem,
        scratch_shapes=state_scratch,
        cost_estimate=cost(width // 2),
        compiler_params=params,
        name="attend_far_high",
    )(blocks, own, queries, peak, acc, keys, values, marks)
    return low, high


def pack(key_value, order, length):
    def split(v):
        return jnp.stack([v // 64, v % 64])

    facts = jnp.concatenate([split(order), split(jnp.broadcast_to(length, (UNIT,)))]).astype(jnp.bfloat16)
    facts = jnp.pad(facts, ((0, PACKED_ROWS - SHARD_ROWS - 4), (0, 0)))
    return jnp.concatenate([key_value, jnp.broadcast_to(facts, (2,) + facts.shape)], axis=1)


def order_rows(order):
    return jnp.tile(order.reshape(2, HALF).astype(jnp.float32), (1, 2))


AXES = ("zl", "x", "core", "y", "zh")


def turn(axis_value, axis, by, size):
    return lax.ppermute(axis_value, axis, [(i, (i + by) % size) for i in range(size)])


def gather_shards(own):
    rows = own.shape[0] // 2
    left = turn(own, "x", 1, 4)
    right = turn(own, "x", 3, 4)
    above = turn(own, "zl", 1, 2)
    far_low = turn(left[:rows], "x", 1, 4)
    far_high = turn(right[rows:], "x", 3, 4)
    above_left = turn(above, "x", 1, 4)
    above_right = turn(above, "x", 3, 4)
    above_far_low = turn(far_low, "zl", 1, 2)
    above_far_high = turn(far_high, "zl", 1, 2)
    return (own, left, right, far_low, far_high, above, above_left, above_right, above_far_low, above_far_high)


def mate(value):
    return turn(value, "core", 1, 2)


def gather_key_values(own):
    left = turn(own, "x", 1, 4)
    right = turn(own, "x", 3, 4)
    above = turn(own, "zl", 1, 2)
    near = [own, left, right, above]
    far_keys = turn(left[0], "x", 1, 4)
    far_values = turn(right[1], "x", 3, 4)
    far = [turn(above, "x", by, 4) for by in (1, 3, 2)]
    near = near + [mate(shard) for shard in near]
    far = far + [mate(shard) for shard in far]
    return near, far + [far_keys, far_values, mate(far_keys), mate(far_values)]


def project_kernel(place, *refs):
    *shards, weight, out, joined = refs
    tokens = shards[0].shape[0]
    for ref, (spot, begin) in zip(shards, SHARD_SPOTS):
        at = pl.multiple_of(place[spot] * tokens + begin * (tokens // 2), 16)
        joined[pl.ds(at, ref.shape[0]), :] = ref[...]
    out[...] = jnp.dot(joined[...], weight[...], preferred_element_type=jnp.float32).astype(jnp.bfloat16)


SHARD_SPOTS = ((0, 0), (1, 0), (2, 0), (3, 0), (3, 1), (4, 0), (5, 0), (6, 0), (7, 0), (7, 1))


def project(place, shards, weight):
    tokens = 8 * shards[0].shape[0]
    vmem = pl.BlockSpec(memory_space=pltpu.VMEM)
    return pl.pallas_call(
        project_kernel,
        out_shape=jax.ShapeDtypeStruct((tokens, weight.shape[1]), jnp.bfloat16),
        in_specs=[pl.BlockSpec(memory_space=pltpu.SMEM)] + [vmem] * (len(shards) + 1),
        out_specs=vmem,
        scratch_shapes=[pltpu.VMEM((tokens, weight.shape[0]), jnp.bfloat16)],
        cost_estimate=pl.CostEstimate(
            flops=2 * tokens * weight.shape[0] * weight.shape[1],
            bytes_accessed=2 * (tokens + weight.shape[1]) * weight.shape[0],
            transcendentals=0,
        ),
        compiler_params=pltpu.CompilerParams(vmem_limit_bytes=40 * 2**20),
    )(place, *shards, weight)


def scatter_sum(terms, y, zh):
    pieces = terms.reshape(4, 2, -1, terms.shape[1])

    def piece(k):
        return lax.dynamic_index_in_dim(pieces, (y + k) % 4, 0, keepdims=False)

    parts = [turn(piece(k), "y", k, 4) for k in (1, 3, 2)]
    total = piece(0).astype(jnp.float32)
    for part in parts:
        total = total + part.astype(jnp.float32)
    away = turn(lax.dynamic_index_in_dim(total, 1 - zh, 0, keepdims=False).astype(jnp.bfloat16), "zh", 1, 2)
    kept = lax.dynamic_index_in_dim(total, zh, 0, keepdims=False)
    return (kept + away.astype(jnp.float32)).astype(jnp.bfloat16)


def body(queries, key_value_cache, cache_lengths, token_order, out_weight):
    zl, x, core, y, zh = (lax.axis_index(name) for name in AXES)
    own = pack(key_value_cache, token_order, cache_lengths)
    near, far = gather_key_values(own)
    late_weight, near[-1] = lax.optimization_barrier((out_weight, near[-1]))
    other_weight = turn(late_weight, "core", 1, 2)
    halves = attend(order_rows(token_order), queries, near, far)
    rows = [zl * 4 + (x + d) % 4 for d in (0, 3, 1, 2)]
    place = jnp.stack(rows + [(row + 4) % 8 for row in rows]).astype(jnp.int32)
    own_parts, other_parts = [], []
    for half in halves:
        shards = gather_shards(half)
        other_parts.append(turn(scatter_sum(project(place, shards, other_weight), y, zh), "core", 1, 2))
        own_parts.append(scatter_sum(project(place, shards, out_weight), y, zh))
    own_rows = jnp.concatenate(own_parts, axis=0)
    other_rows = jnp.concatenate(other_parts, axis=0)
    first = jnp.where(core == 0, own_rows, other_rows)
    second = jnp.where(core == 0, other_rows, own_rows)
    return jnp.concatenate([first, second], axis=0)


def solution(mesh):
    torus = Mesh(mesh.devices.reshape(2, 4, 2, 4, 2), AXES)
    ctx, tp = ("zl", "x", "core"), ("y", "zh")
    return jax.shard_map(
        body,
        mesh=torus,
        in_specs=(P(ctx, tp), P(None, ctx, tp), P(ctx), P(ctx), P(tp, ctx)),
        out_specs=P(tp, ctx),
        check_vma=False,
    )
```
